32 devices in a mesh: problem: 1 (over z), samp: 4 (over y), feat: 8 (over x, core).
Axes of the slice: x: 4, y: 4, z: 1, core: 2. Of those that a mesh axis runs over, the one named last changes fastest.
The devices are a block of a 4x4x8 slice.
Arguments:
- design: bfloat16 [512, 1048576], P(('problem', 'samp'), 'feat')
- targets: float32 [512, 32], P(('problem', 'samp'))
- coef_init: float32 [1048576, 32], P(('problem', 'feat'))
- step_sizes: float32 [1048576], P(('problem', 'feat'))
- ridge_weights: float32 [32], P('problem')
Outputs:
- output 1: float32 [1048576, 32], P(('problem', 'feat'))
- output 2: float32 [512, 32], P(('problem', 'samp'))
All inputs are finite; a program needn't handle non-finite values.
Results may differ from the reference program's by a relative error of at most 0.00635085.
Values are sent between devices in bfloat16 or wider.
A program may use at most 768 MiB of HBM per device.

```python
import jax
import jax.numpy as jnp
from jax import lax

NUM_ROWS = 512
NUM_FEATURES = 1048576
NUM_TARGETS = 32
FEAT_BLOCKS = 8
SWEEPS = 4
STEP_WEIGHT = 0.5


def setup_inputs(seed: int = 0, part: int = 0) -> dict:
    base_key = jax.random.fold_in(jax.random.key(seed), part)
    sub_keys = jax.random.split(base_key, 9)
    shared_rank = 8
    shared_mix = 0.8
    row_block = NUM_ROWS // 8
    factors = jax.random.normal(sub_keys[0], (NUM_ROWS, shared_rank), jnp.float32)
    loadings = jax.random.normal(sub_keys[1], (shared_rank, NUM_FEATURES), jnp.float32)

    def draw_rows(block_index):
        rows_f = lax.dynamic_slice_in_dim(factors, block_index * row_block, row_block, 0)
        shared = jnp.dot(rows_f, loadings) * (shared_mix / shared_rank) ** 0.5
        noise_blk = jax.random.normal(jax.random.fold_in(sub_keys[2], block_index), (row_block, NUM_FEATURES), jnp.float32)
        return (shared + (1.0 - shared_mix) ** 0.5 * noise_blk).astype(jnp.bfloat16)

    design = lax.map(draw_rows, jnp.arange(8)).reshape(NUM_ROWS, NUM_FEATURES)

    def power_step(step_index, probe_vec):
        unit_vec = probe_vec / jnp.linalg.norm(probe_vec)
        image_vec = jnp.dot(design, unit_vec.astype(jnp.bfloat16), preferred_element_type=jnp.float32)
        return jnp.dot(image_vec.astype(jnp.bfloat16), design, preferred_element_type=jnp.float32) / NUM_ROWS

    probe_init = jax.random.normal(sub_keys[3], (NUM_FEATURES,), jnp.float32)
    curvature = 1.15 * jnp.linalg.norm(lax.fori_loop(0, 12, power_step, probe_init))
    step_sizes = jax.random.uniform(sub_keys[4], (NUM_FEATURES,), jnp.float32, 0.4, 0.8) / curvature
    ridge_weights = jax.random.uniform(sub_keys[5], (NUM_TARGETS,), jnp.float32, 0.05, 0.25) * curvature
    coef_init = jax.random.normal(sub_keys[6], (NUM_FEATURES, NUM_TARGETS), jnp.float32) * NUM_FEATURES ** -0.5
    w_star = jax.random.normal(sub_keys[7], (NUM_FEATURES, NUM_TARGETS), jnp.float32) * NUM_FEATURES ** -0.5
    targets = jnp.dot(design, w_star.astype(jnp.bfloat16), preferred_element_type=jnp.float32) + 0.3 * jax.random.normal(sub_keys[8], (NUM_ROWS, NUM_TARGETS), jnp.float32)
    return {"design": design, "targets": targets, "coef_init": coef_init, "step_sizes": step_sizes, "ridge_weights": ridge_weights}


def reference(design, targets, coef_init, step_sizes, ridge_weights):
    block_cols = NUM_FEATURES // FEAT_BLOCKS

    def block_sum(weights):
        weights_b = weights.astype(jnp.bfloat16)

        def add_block(acc_sum, block_index):
            col_block = lax.dynamic_slice_in_dim(design, block_index * block_cols, block_cols, 1)
            rows_w = lax.dynamic_slice_in_dim(weights_b, block_index * block_cols, block_cols, 0)
            product = jnp.dot(col_block, rows_w, preferred_element_type=jnp.float32)
            return acc_sum + product.astype(jnp.bfloat16).astype(jnp.float32), None

        return lax.scan(add_block, jnp.zeros((NUM_ROWS, NUM_TARGETS), jnp.float32), jnp.arange(FEAT_BLOCKS))[0]

    def sweep_once(sweep_state, unused):
        coef_cur, resid_cur = sweep_state
        gradient = lax.dot_general(design, resid_cur.astype(jnp.bfloat16), (((0,), (0,)), ((), ())), preferred_element_type=jnp.float32) / NUM_ROWS
        step_delta = step_sizes[:, None] * (gradient - ridge_weights[None, :] * coef_cur)
        return (coef_cur + STEP_WEIGHT * step_delta, resid_cur - STEP_WEIGHT * block_sum(step_delta)), None

    start_state = (coef_init, targets - block_sum(coef_init))
    final_state = lax.scan(sweep_once, start_state, None, length=SWEEPS)[0]
    return final_state[0], final_state[1]
```

```python
import functools

import jax
import jax.numpy as jnp
from jax import lax
from jax.experimental import pallas as pl
from jax.experimental.pallas import tpu as pltpu
from jax.sharding import PartitionSpec as P

SWEEPS = 4
STEP_WEIGHT = 0.5
CHUNK = 1024
AHEAD = 6
STREAM = 4096
STREAM_BUFS = 4
GATHER_FIRST = 8
GATHER_AHEAD = 16
MESH = pl.DeviceIdType.MESH


def sweeps_kernel(
    ns, nf, total_rows,
    x_hbm, y_ref, w0_hbm, eta_hbm, lam_ref,
    wout_hbm, rout_ref,
    xs, relay, ws, eta, acc, sx, sw, p1s, p1, p2, rb,
    x_sem, xsend_sem, relay_sem, w_sem, eta_sem, sx_sem, sw_sem,
    p1_sem, p1s_sem, p2_sem, p2s_sem, p3_sem, p3s_sem,
    gd_sem, gf_sem, gs_sem,
):
    nch, rows_all, cc = xs.shape
    rows = rows_all // ns
    half = rows // 2
    targets = y_ref.shape[0]
    thalf = targets // 2
    quarter = nch * cc
    nstream = x_hbm.shape[1] // STREAM
    s = lax.axis_index("samp")
    f = lax.axis_index("feat")
    right, left, opp = lax.rem(s + 1, ns), lax.rem(s + ns - 1, ns), lax.rem(s + 2, ns)
    samp_peers = [lax.rem(s + k, ns) for k in range(1, ns)]
    feat_peers = [lax.rem(f + k, nf) for k in range(1, nf)]

    def remote(src, dst, send_sem, recv_sem, **where):
        return pltpu.make_async_remote_copy(
            src_ref=src, dst_ref=dst, send_sem=send_sem, recv_sem=recv_sem,
            device_id=where, device_id_type=MESH)

    def cols(owner, c):
        return pl.ds(pl.multiple_of(owner * quarter + c * cc, cc), cc)

    def wait_bytes(ref, sem):
        pltpu.make_async_copy(ref, ref, sem).wait()

    barrier = pltpu.get_barrier_semaphore()
    for peer in samp_peers:
        pl.semaphore_signal(barrier, inc=1, device_id={"samp": peer}, device_id_type=MESH)
    for peer in feat_peers:
        pl.semaphore_signal(barrier, inc=1, device_id={"feat": peer}, device_id_type=MESH)
    pl.semaphore_wait(barrier, ns - 1 + nf - 1)

    def issue_first(c):
        for part, peer in ((0, right), (1, left)):
            remote(x_hbm.at[pl.ds(part * half, half), cols(opp, c)], relay.at[c, part],
                   xsend_sem.at[c], relay_sem.at[c], samp=peer).start()

    def issue_direct(c):
        mine = pl.ds(pl.multiple_of(s * rows, rows), rows)
        for peer in (right, left):
            remote(x_hbm.at[:, cols(peer, c)], xs.at[c, mine, :],
                   xsend_sem.at[c], x_sem.at[c], samp=peer).start()
        pltpu.make_async_copy(x_hbm.at[:, cols(s, c)], xs.at[c, mine, :], x_sem.at[c]).start()
        pltpu.make_async_copy(w0_hbm.at[:, cols(s, c)], ws.at[c], w_sem.at[c]).start()

    def forward(c):
        wait_bytes(relay.at[c], relay_sem.at[c])
        remote(relay.at[c, 0], xs.at[c, pl.ds(pl.multiple_of(left * rows, rows), half), :],
               xsend_sem.at[c], x_sem.at[c], samp=right).start()
        remote(relay.at[c, 1], xs.at[c, pl.ds(pl.multiple_of(right * rows + half, half), half), :],
               xsend_sem.at[c], x_sem.at[c], samp=left).start()

    def stream_copies(i):
        slot = lax.rem(i, STREAM_BUFS)
        span = pl.ds(pl.multiple_of(i * STREAM, STREAM), STREAM)
        return (pltpu.make_async_copy(x_hbm.at[:, span], sx.at[slot], sx_sem.at[slot]),
                pltpu.make_async_copy(w0_hbm.at[:, span], sw.at[slot], sw_sem.at[slot]))

    issue_first(0)
    for i in range(STREAM_BUFS - 1):
        for copy in stream_copies(i):
            copy.start()

    def issue_step(c, carry):
        issue_first(c + 1)
        issue_direct(c)
        return carry

    lax.fori_loop(0, AHEAD, issue_step, 0)
    eta_copy = pltpu.make_async_copy(
        eta_hbm.at[:, pl.ds(pl.multiple_of(s * quarter, quarter), quarter)], eta, eta_sem)
    eta_copy.start()

    contract_last = (((1,), (1,)), ((), ()))

    def first_product(i, total):
        @pl.when(i + STREAM_BUFS - 1 < nstream)
        def _():
            for copy in stream_copies(i + STREAM_BUFS - 1):
                copy.start()

        for copy in stream_copies(i):
            copy.wait()
        slot = lax.rem(i, STREAM_BUFS)
        return total + lax.dot_general(
            sw[slot].astype(jnp.bfloat16), sx[slot], contract_last, preferred_element_type=jnp.float32)

    block_rows = lax.fori_loop(0, nstream, first_product, jnp.zeros((targets, rows), jnp.float32))

    def sum_blocks(r, block_rows):
        p2[r, f] = block_rows.astype(jnp.bfloat16)
        copies = [remote(p2.at[r, f], p2.at[r, f], p2s_sem.at[r], p2_sem.at[r], feat=peer) for peer in feat_peers]
        for copy in copies:
            copy.start()
        wait_bytes(p2.at[r, pl.ds(0, nf - 1)], p2_sem.at[r])
        wait_bytes(p2.at[r, pl.ds(0, nf - 1)], p2s_sem.at[r])
        total = p2[r, 0].astype(jnp.float32)
        for j in range(1, nf):
            total = total + p2[r, j].astype(jnp.float32)
        return total

    def share_resid(r, resid):
        rb[r, s] = resid.astype(jnp.bfloat16)
        for peer in samp_peers:
            remote(rb.at[r, s], rb.at[r, s], p3s_sem.at[r], p3_sem.at[r], samp=peer).start()
        wait_bytes(rb.at[r, pl.ds(0, ns - 1)], p3_sem.at[r])
        wait_bytes(rb.at[r, pl.ds(0, ns - 1)], p3s_sem.at[r])
        return jnp.concatenate([rb[r, q] for q in range(ns)], axis=1)

    def scatter_start(r):
        for q in range(ns):
            p1s[r - 1, q] = acc[:, q * rows:(q + 1) * rows]
        for peer in samp_peers:
            remote(p1s.at[r - 1, peer], p1.at[r - 1, s], p1s_sem.at[r - 1], p1_sem.at[r - 1], samp=peer).start()
        p1[r - 1, s] = p1s[r - 1, s]

    def scatter_done(r):
        wait_bytes(p1.at[r - 1, pl.ds(0, ns - 1)], p1_sem.at[r - 1])
        wait_bytes(p1.at[r - 1, pl.ds(0, ns - 1)], p1s_sem.at[r - 1])
        total = p1[r - 1, 0]
        for q in range(1, ns):
            total = total + p1[r - 1, q]
        return total

    resid = y_ref[...] - sum_blocks(0, block_rows)
    resid_b = share_resid(0, resid)

    diag = lax.broadcasted_iota(jnp.int32, (targets, targets), 0) == lax.broadcasted_iota(
        jnp.int32, (targets, targets), 1)
    ridge = jnp.sum(jnp.where(diag, jnp.broadcast_to(lam_ref[...], (targets, targets)), 0.0), axis=1, keepdims=True)
    eta_copy.wait()

    def sweep_chunk(c, resid_b):
        xc = xs[c]
        grad = jnp.dot(resid_b, xc, preferred_element_type=jnp.float32) / total_rows
        w = ws[c]
        step = eta[:, pl.ds(pl.multiple_of(c * cc, cc), cc)] * (grad - ridge * w)
        ws[c] = w + STEP_WEIGHT * step
        acc[...] += lax.dot_general(step.astype(jnp.bfloat16), xc, contract_last, preferred_element_type=jnp.float32)

    acc[...] = jnp.zeros_like(acc)
    forward(0)

    def sweep_first(c, carry):
        @pl.when(c + AHEAD + 1 < nch)
        def _():
            issue_first(c + AHEAD + 1)

        @pl.when(c + AHEAD < nch)
        def _():
            issue_direct(c + AHEAD)

        @pl.when(c + 1 < nch)
        def _():
            forward(c + 1)

        wait_bytes(xs.at[c], x_sem.at[c])
        wait_bytes(ws.at[c], w_sem.at[c])
        sweep_chunk(c, resid_b)
        return carry

    lax.fori_loop(0, nch, sweep_first, 0)

    def close_sweep(r, resid):
        scatter_start(r)
        return resid - STEP_WEIGHT * sum_blocks(r, scatter_done(r))

    for r in range(1, SWEEPS - 1):
        resid = close_sweep(r, resid)
        resid_b = share_resid(r, resid)
        acc[...] = jnp.zeros_like(acc)

        def sweep_middle(c, carry):
            sweep_chunk(c, resid_b)
            return carry

        lax.fori_loop(0, nch, sweep_middle, 0)

    resid = close_sweep(SWEEPS - 1, resid)
    resid_b = share_resid(SWEEPS - 1, resid)
    acc[...] = jnp.zeros_like(acc)

    def gather_direct(c):
        dst = wout_hbm.at[:, cols(s, c)]
        for peer in (right, left):
            remote(ws.at[c], dst, gs_sem.at[c], gd_sem.at[c], samp=peer).start()
        pltpu.make_async_copy(ws.at[c], dst, gs_sem.at[c]).start()

    def gather_forward(c):
        wait_bytes(wout_hbm.at[:, pl.ds(0, 2 * cc)], gd_sem.at[c])
        upper, lower = pl.ds(0, thalf), pl.ds(thalf, thalf)
        remote(wout_hbm.at[upper, cols(left, c)], wout_hbm.at[upper, cols(left, c)],
               gs_sem.at[c], gf_sem.at[c], samp=right).start()
        remote(wout_hbm.at[lower, cols(right, c)], wout_hbm.at[lower, cols(right, c)],
               gs_sem.at[c], gf_sem.at[c], samp=left).start()

    def sweep_last(c, carry):
        @pl.when((c > 0) & (c <= GATHER_FIRST))
        def _():
            gather_direct(c - 1)

        sweep_chunk(c, resid_b)
        return carry

    lax.fori_loop(0, nch, sweep_last, 0)
    scatter_start(SWEEPS)

    def gather_more(c, carry):
        gather_direct(c)
        return carry

    lax.fori_loop(GATHER_FIRST, GATHER_AHEAD, gather_more, 0)
    rout_ref[...] = resid - STEP_WEIGHT * sum_blocks(SWEEPS, scatter_done(SWEEPS))

    def gather_step(c, carry):
        gather_forward(c)

        @pl.when(c + GATHER_AHEAD < nch)
        def _():
            gather_direct(c + GATHER_AHEAD)

        return carry

    lax.fori_loop(0, nch, gather_step, 0)

    def drain(c, carry):
        wait_bytes(xs.at[c], xsend_sem.at[c])
        wait_bytes(wout_hbm.at[:, pl.ds(0, cc)], gf_sem.at[c])
        wait_bytes(wout_hbm.at[:, pl.ds(0, 4 * cc)], gs_sem.at[c])
        return carry

    lax.fori_loop(0, nch, drain, 0)


def solution(mesh):
    ns, nf = mesh.shape["samp"], mesh.shape["feat"]
    design_spec = P(("problem", "samp"), "feat")
    rows_spec = P(("problem", "samp"), None)
    coef_spec = P(("problem", "feat"), None)
    step_spec = P(("problem", "feat"))
    ridge_spec = P("problem")

    def local_sweeps(design, targets, coef_init, step_sizes, ridge_weights):
        rows, width = design.shape
        nt = targets.shape[1]
        quarter = width // ns
        nch = quarter // CHUNK
        dma = pltpu.SemaphoreType.DMA
        any_spec = pl.BlockSpec(memory_space=pl.ANY)
        vmem_spec = pl.BlockSpec(memory_space=pltpu.VMEM)
        coef_t, resid_t = pl.pallas_call(
            functools.partial(sweeps_kernel, ns, nf, rows * ns),
            out_shape=(jax.ShapeDtypeStruct((nt, width), jnp.float32),
                       jax.ShapeDtypeStruct((nt, rows), jnp.float32)),
            in_specs=[any_spec, vmem_spec, any_spec, any_spec, vmem_spec],
            out_specs=(any_spec, vmem_spec),
            scratch_shapes=[
                pltpu.VMEM((nch, rows * ns, CHUNK), jnp.bfloat16),
                pltpu.VMEM((nch, 2, rows // 2, CHUNK), jnp.bfloat16),
                pltpu.VMEM((nch, nt, CHUNK), jnp.float32),
                pltpu.VMEM((1, quarter), jnp.float32),
                pltpu.VMEM((nt, rows * ns), jnp.float32),
                pltpu.VMEM((STREAM_BUFS, rows, STREAM), jnp.bfloat16),
                pltpu.VMEM((STREAM_BUFS, nt, STREAM), jnp.float32),
                pltpu.VMEM((SWEEPS, ns, nt, rows), jnp.float32),
                pltpu.VMEM((SWEEPS, ns, nt, rows), jnp.float32),
                pltpu.VMEM((SWEEPS + 1, nf, nt, rows), jnp.bfloat16),
                pltpu.VMEM((SWEEPS, ns, nt, rows), jnp.bfloat16),
                dma((nch,)), dma((nch,)), dma((nch,)), dma((nch,)), dma, dma((STREAM_BUFS,)), dma((STREAM_BUFS,)),
                dma((SWEEPS,)), dma((SWEEPS,)), dma((SWEEPS + 1,)), dma((SWEEPS + 1,)), dma((SWEEPS,)), dma((SWEEPS,)),
                dma((nch,)), dma((nch,)), dma((nch,)),
            ],
            compiler_params=pltpu.CompilerParams(
                collective_id=0, has_side_effects=True, vmem_limit_bytes=66 * 1024 * 1024 - 2 * 1024 * 1024 - 65536),
            name="sweeps",
        )(design, targets.T, coef_init.T, step_sizes[None, :], ridge_weights[None, :])
        return coef_t.T, resid_t.T

    return jax.shard_map(
        local_sweeps, mesh=mesh, in_specs=(design_spec, rows_spec, coef_spec, step_spec, ridge_spec),
        out_specs=(coef_spec, rows_spec), check_vma=False)
```

```python
import functools

import jax
import jax.numpy as jnp
from jax import lax
from jax.experimental import pallas as pl
from jax.experimental.pallas import tpu as pltpu
from jax.sharding import PartitionSpec as P

SWEEPS = 4
STEP_WEIGHT = 0.5
CHUNK = 2048
AHEAD = 4
STREAM = 4096
STREAM_BUFS = 3
GATHER_FIRST = 4
GATHER_AHEAD = 8
MESH = pl.DeviceIdType.MESH


def sweeps_kernel(
    ns, nf, total_rows,
    x_hbm, y_ref, w0_hbm, eta_hbm, lam_ref,
    wout, rout_ref,
    xs, eta, acc, sx, sw, p1s, p1, p2, rb,
    x_sem, xsend_sem, w_sem, eta_sem, sx_sem, sw_sem,
    p1_sem, p1s_sem, p2_sem, p2s_sem, p3_sem, p3s_sem,
    gd_sem, gf_sem, gs_sem,
):
    nch, rows_all, cc = xs.shape
    rows = rows_all // ns
    targets = y_ref.shape[0]
    thalf = targets // 2
    quarter = nch * cc
    nstream = x_hbm.shape[1] // STREAM
    s = lax.axis_index("samp")
    f = lax.axis_index("feat")
    right, left, opp = lax.rem(s + 1, ns), lax.rem(s + ns - 1, ns), lax.rem(s + 2, ns)
    samp_peers = [lax.rem(s + k, ns) for k in range(1, ns)]
    feat_peers = [lax.rem(f + k, nf) for k in range(1, nf)]

    def remote(src, dst, send_sem, recv_sem, **where):
        return pltpu.make_async_remote_copy(
            src_ref=src, dst_ref=dst, send_sem=send_sem, recv_sem=recv_sem,
            device_id=where, device_id_type=MESH)

    def cols(owner, c):
        return pl.ds(pl.multiple_of(owner * quarter + c * cc, cc), cc)

    def wait_bytes(ref, sem):
        pltpu.make_async_copy(ref, ref, sem).wait()

    barrier = pltpu.get_barrier_semaphore()
    for peer in samp_peers:
        pl.semaphore_signal(barrier, inc=1, device_id={"samp": peer}, device_id_type=MESH)
    for peer in feat_peers:
        pl.semaphore_signal(barrier, inc=1, device_id={"feat": peer}, device_id_type=MESH)
    pl.semaphore_wait(barrier, ns - 1 + nf - 1)

    def issue(c):
        mine = pl.ds(pl.multiple_of(s * rows, rows), rows)
        for peer in (opp, right, left):
            remote(x_hbm.at[:, cols(peer, c)], xs.at[c, mine, :], xsend_sem.at[c], x_sem.at[c], samp=peer).start()
        pltpu.make_async_copy(x_hbm.at[:, cols(s, c)], xs.at[c, mine, :], x_sem.at[c]).start()
        pltpu.make_async_copy(w0_hbm.at[:, cols(s, c)], wout.at[:, cols(s, c)], w_sem.at[c]).start()

    def stream_copies(i):
        slot = lax.rem(i, STREAM_BUFS)
        span = pl.ds(pl.multiple_of(i * STREAM, STREAM), STREAM)
        return (pltpu.make_async_copy(x_hbm.at[:, span], sx.at[slot], sx_sem.at[slot]),
                pltpu.make_async_copy(w0_hbm.at[:, span], sw.at[slot], sw_sem.at[slot]))

    for i in range(STREAM_BUFS - 1):
        for copy in stream_copies(i):
            copy.start()

    def issue_step(c, carry):
        issue(c)
        return carry

    lax.fori_loop(0, AHEAD, issue_step, 0)
    eta_copy = pltpu.make_async_copy(
        eta_hbm.at[:, pl.ds(pl.multiple_of(s * quarter, quarter), quarter)], eta, eta_sem)
    eta_copy.start()

    contract_last = (((1,), (1,)), ((), ()))

    def first_product(i, total):
        @pl.when(i + STREAM_BUFS - 1 < nstream)
        def _():
            for copy in stream_copies(i + STREAM_BUFS - 1):
                copy.start()

        for copy in stream_copies(i):
            copy.wait()
        slot = lax.rem(i, STREAM_BUFS)
        return total + lax.dot_general(
            sw[slot].astype(jnp.bfloat16), sx[slot], contract_last, preferred_element_type=jnp.float32)

    block_rows = lax.fori_loop(0, nstream, first_product, jnp.zeros((targets, rows), jnp.float32))

    def sum_blocks(r, block_rows):
        p2[r, f] = block_rows.astype(jnp.bfloat16)
        copies = [remote(p2.at[r, f], p2.at[r, f], p2s_sem.at[r], p2_sem.at[r], feat=peer) for peer in feat_peers]
        for copy in copies:
            copy.start()
        wait_bytes(p2.at[r, pl.ds(0, nf - 1)], p2_sem.at[r])
        total = p2[r, 0].astype(jnp.float32)
        for j in range(1, nf):
            total = total + p2[r, j].astype(jnp.float32)
        return total

    def share_resid(r, resid):
        rb[r, s] = resid.astype(jnp.bfloat16)
        for peer in samp_peers:
            remote(rb.at[r, s], rb.at[r, s], p3s_sem.at[r], p3_sem.at[r], samp=peer).start()
        wait_bytes(rb.at[r, pl.ds(0, ns - 1)], p3_sem.at[r])
        return jnp.concatenate([rb[r, q] for q in range(ns)], axis=1)

    def scatter_start(r):
        for q in range(ns):
            p1s[r - 1, q] = acc[:, q * rows:(q + 1) * rows]
        for peer in samp_peers:
            remote(p1s.at[r - 1, peer], p1.at[r - 1, s], p1s_sem.at[r - 1], p1_sem.at[r - 1], samp=peer).start()
        p1[r - 1, s] = p1s[r - 1, s]

    def scatter_done(r):
        wait_bytes(p1.at[r - 1, pl.ds(0, ns - 1)], p1_sem.at[r - 1])
        total = p1[r - 1, 0]
        for q in range(1, ns):
            total = total + p1[r - 1, q]
        return total

    resid = y_ref[...] - sum_blocks(0, block_rows)
    resid_b = share_resid(0, resid)

    diag = lax.broadcasted_iota(jnp.int32, (targets, targets), 0) == lax.broadcasted_iota(
        jnp.int32, (targets, targets), 1)
    ridge = jnp.sum(jnp.where(diag, jnp.broadcast_to(lam_ref[...], (targets, targets)), 0.0), axis=1, keepdims=True)
    eta_copy.wait()

    def sweep_chunk(c, resid_b):
        xc = xs[c]
        grad = jnp.dot(resid_b, xc, preferred_element_type=jnp.float32) / total_rows
        w = wout[:, cols(s, c)]
        step = eta[:, pl.ds(pl.multiple_of(c * cc, cc), cc)] * (grad - ridge * w)
        wout[:, cols(s, c)] = w + STEP_WEIGHT * step
        acc[...] += lax.dot_general(step.astype(jnp.bfloat16), xc, contract_last, preferred_element_type=jnp.float32)

    acc[...] = jnp.zeros_like(acc)

    def sweep_first(c, carry):
        @pl.when(c + AHEAD < nch)
        def _():
            issue(c + AHEAD)

        wait_bytes(xs.at[c], x_sem.at[c])
        wait_bytes(wout.at[:, pl.ds(0, cc)], w_sem.at[c])
        sweep_chunk(c, resid_b)
        return carry

    lax.fori_loop(0, nch, sweep_first, 0)

    def close_sweep(r, resid):
        scatter_start(r)
        return resid - STEP_WEIGHT * sum_blocks(r, scatter_done(r))

    for r in range(1, SWEEPS - 1):
        resid = close_sweep(r, resid)
        resid_b = share_resid(r, resid)
        acc[...] = jnp.zeros_like(acc)

        def sweep_middle(c, carry):
            sweep_chunk(c, resid_b)
            return carry

        lax.fori_loop(0, nch, sweep_middle, 0)

    resid = close_sweep(SWEEPS - 1, resid)
    resid_b = share_resid(SWEEPS - 1, resid)
    acc[...] = jnp.zeros_like(acc)

    def gather_direct(c):
        mine = wout.at[:, cols(s, c)]
        for peer in (right, left):
            remote(mine, mine, gs_sem.at[c], gd_sem.at[c], samp=peer).start()

    def gather_forward(c):
        wait_bytes(wout.at[:, pl.ds(0, 2 * cc)], gd_sem.at[c])
        for part, peer, origin in ((0, right, left), (1, left, right)):
            theirs = wout.at[pl.ds(part * thalf, thalf), cols(origin, c)]
            remote(theirs, theirs, gs_sem.at[c], gf_sem.at[c], samp=peer).start()

    def sweep_last(c, carry):
        @pl.when((c > 0) & (c <= GATHER_FIRST))
        def _():
            gather_direct(c - 1)

        sweep_chunk(c, resid_b)
        return carry

    lax.fori_loop(0, nch, sweep_last, 0)
    scatter_start(SWEEPS)

    def gather_more(c, carry):
        gather_direct(c)
        return carry

    lax.fori_loop(GATHER_FIRST, GATHER_AHEAD, gather_more, 0)
    rout_ref[...] = resid - STEP_WEIGHT * sum_blocks(SWEEPS, scatter_done(SWEEPS))

    def gather_step(c, carry):
        gather_forward(c)

        @pl.when(c + GATHER_AHEAD < nch)
        def _():
            gather_direct(c + GATHER_AHEAD)

        return carry

    lax.fori_loop(0, nch, gather_step, 0)

    def drain(c, carry):
        wait_bytes(xs.at[c, pl.ds(0, rows_all - rows)], xsend_sem.at[c])
        wait_bytes(wout.at[:, pl.ds(0, cc)], gf_sem.at[c])
        wait_bytes(wout.at[:, pl.ds(0, 3 * cc)], gs_sem.at[c])
        return carry

    lax.fori_loop(0, nch, drain, 0)
    for r in range(SWEEPS + 1):
        wait_bytes(p2.at[r, pl.ds(0, nf - 1)], p2s_sem.at[r])
    for r in range(SWEEPS):
        wait_bytes(rb.at[r, pl.ds(0, ns - 1)], p3s_sem.at[r])
        wait_bytes(p1.at[r, pl.ds(0, ns - 1)], p1s_sem.at[r])


def solution(mesh):
    ns, nf = mesh.shape["samp"], mesh.shape["feat"]
    design_spec = P(("problem", "samp"), "feat")
    rows_spec = P(("problem", "samp"), None)
    coef_spec = P(("problem", "feat"), None)
    step_spec = P(("problem", "feat"))
    ridge_spec = P("problem")

    def local_sweeps(design, targets, coef_init, step_sizes, ridge_weights):
        rows, width = design.shape
        nt = targets.shape[1]
        quarter = width // ns
        nch = quarter // CHUNK
        dma = pltpu.SemaphoreType.DMA
        any_spec = pl.BlockSpec(memory_space=pl.ANY)
        vmem_spec = pl.BlockSpec(memory_space=pltpu.VMEM)
        coef_t, resid_t = pl.pallas_call(
            functools.partial(sweeps_kernel, ns, nf, rows * ns),
            out_shape=(pltpu.VMEM((nt, width), jnp.float32),
                       jax.ShapeDtypeStruct((nt, rows), jnp.float32)),
            in_specs=[any_spec, vmem_spec, any_spec, any_spec, vmem_spec],
            out_specs=(vmem_spec, vmem_spec),
            scratch_shapes=[
                pltpu.VMEM((nch, rows * ns, CHUNK), jnp.bfloat16),
                pltpu.VMEM((1, quarter), jnp.float32),
                pltpu.VMEM((nt, rows * ns), jnp.float32),
                pltpu.VMEM((STREAM_BUFS, rows, STREAM), jnp.bfloat16),
                pltpu.VMEM((STREAM_BUFS, nt, STREAM), jnp.float32),
                pltpu.VMEM((SWEEPS, ns, nt, rows), jnp.float32),
                pltpu.VMEM((SWEEPS, ns, nt, rows), jnp.float32),
                pltpu.VMEM((SWEEPS + 1, nf, nt, rows), jnp.bfloat16),
                pltpu.VMEM((SWEEPS, ns, nt, rows), jnp.bfloat16),
                dma((nch,)), dma((nch,)), dma((nch,)), dma, dma((STREAM_BUFS,)), dma((STREAM_BUFS,)),
                dma((SWEEPS,)), dma((SWEEPS,)), dma((SWEEPS + 1,)), dma((SWEEPS + 1,)), dma((SWEEPS,)), dma((SWEEPS,)),
                dma((nch,)), dma((nch,)), dma((nch,)),
            ],
            compiler_params=pltpu.CompilerParams(
                collective_id=0, has_side_effects=True, vmem_limit_bytes=47 * 1024 * 1024),
            name="sweeps",
        )(design, targets.T, coef_init.T, step_sizes[None, :], ridge_weights[None, :])
        return coef_t.T, resid_t.T

    return jax.shard_map(
        local_sweeps, mesh=mesh, in_specs=(design_spec, rows_spec, coef_spec, step_spec, ridge_spec),
        out_specs=(coef_spec, rows_spec), check_vma=False)
```

```python
import functools

import jax
import jax.numpy as jnp
from jax import lax
from jax.experimental import pallas as pl
from jax.experimental.pallas import tpu as pltpu
from jax.sharding import PartitionSpec as P

SWEEPS = 4
STEP_WEIGHT = 0.5
CHUNK = 2048
AHEAD = 4
STREAM = 4096
STREAM_BUFS = 3
GATHER_FIRST = 4
GATHER_AHEAD = 8
UNROLL = 4
MESH = pl.DeviceIdType.MESH


def sweeps_kernel(
    ns, nf, total_rows,
    x_hbm, y_ref, w0_hbm, eta_hbm, lam_ref,
    wout, rout_ref,
    xs, eta, acc, sx, sw, p1s, p1, p2, pm, rs,
    x_sem, xsend_sem, w_sem, eta_sem, sx_sem, sw_sem,
    p1_sem, p1s_sem, p2_sem, p2s_sem, pm_sem, pms_sem, rs_sem, rss_sem,
    gd_sem, gf_sem, gs_sem,
):
    nch, rows_all, cc = xs.shape
    rows = rows_all // ns
    targets = y_ref.shape[0]
    thalf = targets // 2
    quarter = nch * cc
    nstream = x_hbm.shape[1] // STREAM
    s = lax.axis_index("samp")
    f = lax.axis_index("feat")
    right, left, opp = lax.rem(s + 1, ns), lax.rem(s + ns - 1, ns), lax.rem(s + 2, ns)
    samp_peers = [opp, right, left]
    feat_peers = [lax.rem(f + k, nf) for k in range(1, nf)]
    far_first = sorted(((i, j) for i in range(ns) for j in range(nf) if i or j),
                       key=lambda d: -min(d[0], ns - d[0]) - min(d[1], nf - d[1]) / 2)
    group = [{"samp": lax.rem(s + i, ns), "feat": lax.rem(f + j, nf)} for i, j in far_first]

    def remote(src, dst, send_sem, recv_sem, **where):
        return pltpu.make_async_remote_copy(
            src_ref=src, dst_ref=dst, send_sem=send_sem, recv_sem=recv_sem,
            device_id=where, device_id_type=MESH)

    def cols(owner, c):
        return pl.ds(pl.multiple_of(owner * quarter + c * cc, cc), cc)

    def wait_bytes(ref, sem):
        pltpu.make_async_copy(ref, ref, sem).wait()

    barrier = pltpu.get_barrier_semaphore()
    for peer in group:
        pl.semaphore_signal(barrier, inc=1, device_id=peer, device_id_type=MESH)
    pl.semaphore_wait(barrier, len(group))

    def issue(c):
        mine = pl.ds(pl.multiple_of(s * rows, rows), rows)
        for peer in (opp, right, left):
            remote(x_hbm.at[:, cols(peer, c)], xs.at[c, mine, :], xsend_sem.at[c], x_sem.at[c], samp=peer).start()
        pltpu.make_async_copy(x_hbm.at[:, cols(s, c)], xs.at[c, mine, :], x_sem.at[c]).start()
        pltpu.make_async_copy(w0_hbm.at[:, cols(s, c)], wout.at[:, cols(s, c)], w_sem.at[c]).start()

    def stream_copies(i):
        slot = lax.rem(i, STREAM_BUFS)
        span = pl.ds(pl.multiple_of(i * STREAM, STREAM), STREAM)
        return (pltpu.make_async_copy(x_hbm.at[:, span], sx.at[slot], sx_sem.at[slot]),
                pltpu.make_async_copy(w0_hbm.at[:, span], sw.at[slot], sw_sem.at[slot]))

    for i in range(STREAM_BUFS - 1):
        for copy in stream_copies(i):
            copy.start()

    def issue_step(c, carry):
        issue(c)
        return carry

    lax.fori_loop(0, AHEAD, issue_step, 0)
    eta_copy = pltpu.make_async_copy(
        eta_hbm.at[:, pl.ds(pl.multiple_of(s * quarter, quarter), quarter)], eta, eta_sem)
    eta_copy.start()

    contract_last = (((1,), (1,)), ((), ()))

    def first_product(i, total):
        @pl.when(i + STREAM_BUFS - 1 < nstream)
        def _():
            for copy in stream_copies(i + STREAM_BUFS - 1):
                copy.start()

        for copy in stream_copies(i):
            copy.wait()
        slot = lax.rem(i, STREAM_BUFS)
        return total + lax.dot_general(
            sw[slot].astype(jnp.bfloat16), sx[slot], contract_last, preferred_element_type=jnp.float32)

    block_rows = lax.fori_loop(0, nstream, first_product, jnp.zeros((targets, rows), jnp.float32))

    def sum_blocks(r, block_rows):
        p2[r, f] = block_rows.astype(jnp.bfloat16)
        copies = [remote(p2.at[r, f], p2.at[r, f], p2s_sem.at[r], p2_sem.at[r], feat=peer) for peer in feat_peers]
        for copy in copies:
            copy.start()
        wait_bytes(p2.at[r, pl.ds(0, nf - 1)], p2_sem.at[r])
        total = p2[r, 0].astype(jnp.float32)
        for j in range(1, nf):
            total = total + p2[r, j].astype(jnp.float32)
        return total

    def sum_blocks_all(r, block_rows):
        pm[r - 1, s * nf + f] = block_rows.astype(jnp.bfloat16)
        mine = pm.at[r - 1, s * nf + f]
        for peer in group:
            remote(mine, mine, pms_sem.at[r - 1], pm_sem.at[r - 1], **peer).start()
        wait_bytes(pm.at[r - 1, pl.ds(0, ns * nf - 1)], pm_sem.at[r - 1])
        for q in range(ns):
            total = pm[r - 1, q * nf].astype(jnp.float32)
            for j in range(1, nf):
                total = total + pm[r - 1, q * nf + j].astype(jnp.float32)
            rs[q] = rs[q] - STEP_WEIGHT * total

    def rounded_resid():
        return jnp.concatenate([rs[q].astype(jnp.bfloat16) for q in range(ns)], axis=1)

    def scatter_start(r):
        for q in range(ns):
            p1s[r - 1, q] = acc[:, q * rows:(q + 1) * rows]
        for peer in samp_peers:
            remote(p1s.at[r - 1, peer], p1.at[r - 1, s], p1s_sem.at[r - 1], p1_sem.at[r - 1], samp=peer).start()
        p1[r - 1, s] = p1s[r - 1, s]

    def scatter_done(r):
        wait_bytes(p1.at[r - 1, pl.ds(0, ns - 1)], p1_sem.at[r - 1])
        total = p1[r - 1, 0]
        for q in range(1, ns):
            total = total + p1[r - 1, q]
        return total

    rs[s] = y_ref[...] - sum_blocks(0, block_rows)
    for peer in samp_peers:
        remote(rs.at[s], rs.at[s], rss_sem, rs_sem, samp=peer).start()
    wait_bytes(rs.at[pl.ds(0, ns - 1)], rs_sem)
    wait_bytes(rs.at[pl.ds(0, ns - 1)], rss_sem)
    resid_b = rounded_resid()

    diag = lax.broadcasted_iota(jnp.int32, (targets, targets), 0) == lax.broadcasted_iota(
        jnp.int32, (targets, targets), 1)
    ridge = jnp.sum(jnp.where(diag, jnp.broadcast_to(lam_ref[...], (targets, targets)), 0.0), axis=1, keepdims=True)
    eta_copy.wait()

    def sweep_chunk(c, resid_b):
        xc = xs[c]
        grad = jnp.dot(resid_b, xc, preferred_element_type=jnp.float32) / total_rows
        w = wout[:, cols(s, c)]
        step = eta[:, pl.ds(pl.multiple_of(c * cc, cc), cc)] * (grad - ridge * w)
        wout[:, cols(s, c)] = w + STEP_WEIGHT * step
        acc[...] += lax.dot_general(step.astype(jnp.bfloat16), xc, contract_last, preferred_element_type=jnp.float32)

    acc[...] = jnp.zeros_like(acc)

    def sweep_first(c, carry):
        @pl.when(c + AHEAD < nch)
        def _():
            issue(c + AHEAD)

        wait_bytes(xs.at[c], x_sem.at[c])
        wait_bytes(wout.at[:, pl.ds(0, cc)], w_sem.at[c])
        sweep_chunk(c, resid_b)
        return carry

    lax.fori_loop(0, nch, sweep_first, 0)

    def close_sweep(r):
        scatter_start(r)
        sum_blocks_all(r, scatter_done(r))
        acc[...] = jnp.zeros_like(acc)
        return rounded_resid()

    for r in range(1, SWEEPS - 1):
        resid_b = close_sweep(r)

        def sweep_middle(c, carry):
            sweep_chunk(c, resid_b)
            return carry

        lax.fori_loop(0, nch, sweep_middle, 0, unroll=UNROLL)

    resid_b = close_sweep(SWEEPS - 1)

    def gather_direct(c):
        mine = wout.at[:, cols(s, c)]
        for peer in (right, left):
            remote(mine, mine, gs_sem.at[c], gd_sem.at[c], samp=peer).start()

    def gather_forward(c):
        wait_bytes(wout.at[:, pl.ds(0, 2 * cc)], gd_sem.at[c])
        for part, peer, origin in ((0, right, left), (1, left, right)):
            theirs = wout.at[pl.ds(part * thalf, thalf), cols(origin, c)]
            remote(theirs, theirs, gs_sem.at[c], gf_sem.at[c], samp=peer).start()

    def sweep_last(c, carry):
        @pl.when((c > 0) & (c <= GATHER_FIRST))
        def _():
            gather_direct(c - 1)

        sweep_chunk(c, resid_b)
        return carry

    lax.fori_loop(0, nch, sweep_last, 0)
    scatter_start(SWEEPS)

    def gather_more(c, carry):
        gather_direct(c)
        return carry

    lax.fori_loop(GATHER_FIRST, GATHER_AHEAD, gather_more, 0)
    rout_ref[...] = rs[s] - STEP_WEIGHT * sum_blocks(1, scatter_done(SWEEPS))

    def gather_step(c, carry):
        gather_forward(c)

        @pl.when(c + GATHER_AHEAD < nch)
        def _():
            gather_direct(c + GATHER_AHEAD)

        return carry

    lax.fori_loop(0, nch, gather_step, 0)

    def drain(c, carry):
        wait_bytes(xs.at[c, pl.ds(0, rows_all - rows)], xsend_sem.at[c])
        wait_bytes(wout.at[:, pl.ds(0, cc)], gf_sem.at[c])
        wait_bytes(wout.at[:, pl.ds(0, 3 * cc)], gs_sem.at[c])
        return carry

    lax.fori_loop(0, nch, drain, 0)
    for r in range(2):
        wait_bytes(p2.at[r, pl.ds(0, nf - 1)], p2s_sem.at[r])
    for r in range(SWEEPS - 1):
        wait_bytes(pm.at[r, pl.ds(0, ns * nf - 1)], pms_sem.at[r])
    for r in range(SWEEPS):
        wait_bytes(p1.at[r, pl.ds(0, ns - 1)], p1s_sem.at[r])


def solution(mesh):
    ns, nf = mesh.shape["samp"], mesh.shape["feat"]
    design_spec = P(("problem", "samp"), "feat")
    rows_spec = P(("problem", "samp"), None)
    coef_spec = P(("problem", "feat"), None)
    step_spec = P(("problem", "feat"))
    ridge_spec = P("problem")

    def local_sweeps(design, targets, coef_init, step_sizes, ridge_weights):
        rows, width = design.shape
        nt = targets.shape[1]
        quarter = width // ns
        nch = quarter // CHUNK
        dma = pltpu.SemaphoreType.DMA
        any_spec = pl.BlockSpec(memory_space=pl.ANY)
        vmem_spec = pl.BlockSpec(memory_space=pltpu.VMEM)
        coef_t, resid_t = pl.pallas_call(
            functools.partial(sweeps_kernel, ns, nf, rows * ns),
            out_shape=(pltpu.VMEM((nt, width), jnp.float32),
                       jax.ShapeDtypeStruct((nt, rows), jnp.float32)),
            in_specs=[any_spec, vmem_spec, any_spec, any_spec, vmem_spec],
            out_specs=(vmem_spec, vmem_spec),
            scratch_shapes=[
                pltpu.VMEM((nch, rows * ns, CHUNK), jnp.bfloat16),
                pltpu.VMEM((1, quarter), jnp.float32),
                pltpu.VMEM((nt, rows * ns), jnp.float32),
                pltpu.VMEM((STREAM_BUFS, rows, STREAM), jnp.bfloat16),
                pltpu.VMEM((STREAM_BUFS, nt, STREAM), jnp.float32),
                pltpu.VMEM((SWEEPS, ns, nt, rows), jnp.float32),
                pltpu.VMEM((SWEEPS, ns, nt, rows), jnp.float32),
                pltpu.VMEM((2, nf, nt, rows), jnp.bfloat16),
                pltpu.VMEM((SWEEPS - 1, ns * nf, nt, rows), jnp.bfloat16),
                pltpu.VMEM((ns, nt, rows), jnp.float32),
                dma((nch,)), dma((nch,)), dma((nch,)), dma, dma((STREAM_BUFS,)), dma((STREAM_BUFS,)),
                dma((SWEEPS,)), dma((SWEEPS,)), dma((2,)), dma((2,)), dma((SWEEPS - 1,)), dma((SWEEPS - 1,)), dma, dma,
                dma((nch,)), dma((nch,)), dma((nch,)),
            ],
            compiler_params=pltpu.CompilerParams(
                collective_id=0, has_side_effects=True, vmem_limit_bytes=47 * 1024 * 1024),
            name="sweeps",
        )(design, targets.T, coef_init.T, step_sizes[None, :], ridge_weights[None, :])
        return coef_t.T, resid_t.T

    return jax.shard_map(
        local_sweeps, mesh=mesh, in_specs=(design_spec, rows_spec, coef_spec, step_spec, ridge_spec),
        out_specs=(coef_spec, rows_spec), check_vma=False)
```

```python
import functools

import jax
import jax.numpy as jnp
from jax import lax
from jax.experimental import pallas as pl
from jax.experimental.pallas import tpu as pltpu
from jax.sharding import PartitionSpec as P

SWEEPS = 4
STEP_WEIGHT = 0.5
CHUNK = 2048
AHEAD = 4
STREAM = 4096
STREAM_BUFS = 3
GATHER_FIRST = 4
GATHER_AHEAD = 8
UNROLL = 8
MESH = pl.DeviceIdType.MESH


def sweeps_kernel(
    ns, nf, total_rows,
    x_hbm, y_ref, w0_hbm, eta_hbm, lam_ref,
    wout, rout_ref,
    xs, sb, eta, acc, sx, sw, p1s, p1, p2, pm, rs,
    x_sem, xsend_sem, w_sem, eta_sem, sx_sem, sw_sem,
    p1_sem, p1s_sem, p2_sem, p2s_sem, pm_sem, pms_sem, rs_sem, rss_sem,
    gd_sem, gf_sem, gs_sem,
):
    nch, rows_all, cc = xs.shape
    rows = rows_all // ns
    targets = y_ref.shape[0]
    thalf = targets // 2
    quarter = nch * cc
    nstream = x_hbm.shape[1] // STREAM
    s = lax.axis_index("samp")
    f = lax.axis_index("feat")
    right, left, opp = lax.rem(s + 1, ns), lax.rem(s + ns - 1, ns), lax.rem(s + 2, ns)
    samp_peers = [opp, right, left]
    feat_peers = [lax.rem(f + k, nf) for k in range(1, nf)]
    far_first = sorted(((i, j) for i in range(ns) for j in range(nf) if i or j),
                       key=lambda d: -min(d[0], ns - d[0]) - min(d[1], nf - d[1]) / 2)
    group = [{"samp": lax.rem(s + i, ns), "feat": lax.rem(f + j, nf)} for i, j in far_first]

    def remote(src, dst, send_sem, recv_sem, **where):
        return pltpu.make_async_remote_copy(
            src_ref=src, dst_ref=dst, send_sem=send_sem, recv_sem=recv_sem,
            device_id=where, device_id_type=MESH)

    def cols(owner, c):
        return pl.ds(pl.multiple_of(owner * quarter + c * cc, cc), cc)

    def wait_bytes(ref, sem):
        pltpu.make_async_copy(ref, ref, sem).wait()

    barrier = pltpu.get_barrier_semaphore()
    for peer in group:
        pl.semaphore_signal(barrier, inc=1, device_id=peer, device_id_type=MESH)
    pl.semaphore_wait(barrier, len(group))

    def issue(c):
        mine = pl.ds(pl.multiple_of(s * rows, rows), rows)
        for peer in (opp, right, left):
            remote(x_hbm.at[:, cols(peer, c)], xs.at[c, mine, :], xsend_sem.at[c], x_sem.at[c], samp=peer).start()
        pltpu.make_async_copy(x_hbm.at[:, cols(s, c)], xs.at[c, mine, :], x_sem.at[c]).start()
        pltpu.make_async_copy(w0_hbm.at[:, cols(s, c)], wout.at[:, cols(s, c)], w_sem.at[c]).start()

    def stream_copies(i):
        slot = lax.rem(i, STREAM_BUFS)
        span = pl.ds(pl.multiple_of(i * STREAM, STREAM), STREAM)
        return (pltpu.make_async_copy(x_hbm.at[:, span], sx.at[slot], sx_sem.at[slot]),
                pltpu.make_async_copy(w0_hbm.at[:, span], sw.at[slot], sw_sem.at[slot]))

    for i in range(STREAM_BUFS - 1):
        for copy in stream_copies(i):
            copy.start()

    def issue_step(c, carry):
        issue(c)
        return carry

    lax.fori_loop(0, AHEAD, issue_step, 0)
    eta_copy = pltpu.make_async_copy(
        eta_hbm.at[:, pl.ds(pl.multiple_of(s * quarter, quarter), quarter)], eta, eta_sem)
    eta_copy.start()

    contract_last = (((1,), (1,)), ((), ()))

    def first_product(i, total):
        @pl.when(i + STREAM_BUFS - 1 < nstream)
        def _():
            for copy in stream_copies(i + STREAM_BUFS - 1):
                copy.start()

        for copy in stream_copies(i):
            copy.wait()
        slot = lax.rem(i, STREAM_BUFS)
        return total + lax.dot_general(
            sw[slot].astype(jnp.bfloat16), sx[slot], contract_last, preferred_element_type=jnp.float32)

    block_rows = lax.fori_loop(0, nstream, first_product, jnp.zeros((targets, rows), jnp.float32))

    def sum_blocks(r, block_rows):
        p2[r, f] = block_rows.astype(jnp.bfloat16)
        copies = [remote(p2.at[r, f], p2.at[r, f], p2s_sem.at[r], p2_sem.at[r], feat=peer) for peer in feat_peers]
        for copy in copies:
            copy.start()
        wait_bytes(p2.at[r, pl.ds(0, nf - 1)], p2_sem.at[r])
        total = p2[r, 0].astype(jnp.float32)
        for j in range(1, nf):
            total = total + p2[r, j].astype(jnp.float32)
        return total

    def sum_blocks_all(r, block_rows):
        pm[r - 1, s * nf + f] = block_rows.astype(jnp.bfloat16)
        mine = pm.at[r - 1, s * nf + f]
        for peer in group:
            remote(mine, mine, pms_sem.at[r - 1], pm_sem.at[r - 1], **peer).start()
        wait_bytes(pm.at[r - 1, pl.ds(0, ns * nf - 1)], pm_sem.at[r - 1])
        for q in range(ns):
            total = pm[r - 1, q * nf].astype(jnp.float32)
            for j in range(1, nf):
                total = total + pm[r - 1, q * nf + j].astype(jnp.float32)
            rs[q] = rs[q] - STEP_WEIGHT * total

    def rounded_resid():
        return jnp.concatenate([rs[q].astype(jnp.bfloat16) for q in range(ns)], axis=1)

    def scatter_start(r):
        for q in range(ns):
            p1s[r - 1, q] = acc[:, q * rows:(q + 1) * rows]
        for peer in samp_peers:
            remote(p1s.at[r - 1, peer], p1.at[r - 1, s], p1s_sem.at[r - 1], p1_sem.at[r - 1], samp=peer).start()
        p1[r - 1, s] = p1s[r - 1, s]

    def scatter_done(r):
        wait_bytes(p1.at[r - 1, pl.ds(0, ns - 1)], p1_sem.at[r - 1])
        total = p1[r - 1, 0]
        for q in range(1, ns):
            total = total + p1[r - 1, q]
        return total

    rs[s] = y_ref[...] - sum_blocks(0, block_rows)
    for peer in samp_peers:
        remote(rs.at[s], rs.at[s], rss_sem, rs_sem, samp=peer).start()
    wait_bytes(rs.at[pl.ds(0, ns - 1)], rs_sem)
    wait_bytes(rs.at[pl.ds(0, ns - 1)], rss_sem)
    resid_b = rounded_resid()

    diag = lax.broadcasted_iota(jnp.int32, (targets, targets), 0) == lax.broadcasted_iota(
        jnp.int32, (targets, targets), 1)
    ridge = jnp.sum(jnp.where(diag, jnp.broadcast_to(lam_ref[...], (targets, targets)), 0.0), axis=1, keepdims=True)
    eta_copy.wait()

    def sweep_chunk(c, resid_b):
        xc = xs[c]
        grad = jnp.dot(resid_b, xc, preferred_element_type=jnp.float32) / total_rows
        w = wout[:, cols(s, c)]
        step = eta[:, pl.ds(pl.multiple_of(c * cc, cc), cc)] * (grad - ridge * w)
        wout[:, cols(s, c)] = w + STEP_WEIGHT * step
        acc[...] += lax.dot_general(step.astype(jnp.bfloat16), xc, contract_last, preferred_element_type=jnp.float32)

    acc[...] = jnp.zeros_like(acc)

    def sweep_first(c, carry):
        @pl.when(c + AHEAD < nch)
        def _():
            issue(c + AHEAD)

        wait_bytes(xs.at[c], x_sem.at[c])
        wait_bytes(wout.at[:, pl.ds(0, cc)], w_sem.at[c])
        sweep_chunk(c, resid_b)
        return carry

    lax.fori_loop(0, nch, sweep_first, 0)

    def middle_sweep(r, resid_b):
        def step_chunk(c, carry):
            grad = jnp.dot(resid_b, xs[c], preferred_element_type=jnp.float32) / total_rows
            w = wout[:, cols(s, c)]
            step = eta[:, pl.ds(pl.multiple_of(c * cc, cc), cc)] * (grad - ridge * w)
            wout[:, cols(s, c)] = w + STEP_WEIGHT * step
            sb[c] = step.astype(jnp.bfloat16)
            return carry

        lax.fori_loop(0, nch, step_chunk, 0, unroll=UNROLL)

        def block_product(q):
            block = pl.ds(pl.multiple_of(q * rows, rows), rows)
            total = jnp.zeros((rows, targets), jnp.float32)
            for c in range(nch):
                total = total + lax.dot_general(xs[c, block, :], sb[c], contract_last, preferred_element_type=jnp.float32)
            return total.T

        def peer_block(p, carry):
            q = lax.rem(s + 1 + p, ns)
            p1s[r - 1, q] = block_product(q)
            remote(p1s.at[r - 1, q], p1.at[r - 1, s], p1s_sem.at[r - 1], p1_sem.at[r - 1], samp=q).start()
            return carry

        lax.fori_loop(0, ns - 1, peer_block, 0)
        p1[r - 1, s] = block_product(s)

    scatter_start(1)
    sum_blocks_all(1, scatter_done(1))
    for r in range(2, SWEEPS):
        middle_sweep(r, rounded_resid())
        sum_blocks_all(r, scatter_done(r))
    resid_b = rounded_resid()
    acc[...] = jnp.zeros_like(acc)

    def gather_direct(c):
        mine = wout.at[:, cols(s, c)]
        for peer in (right, left):
            remote(mine, mine, gs_sem.at[c], gd_sem.at[c], samp=peer).start()

    def gather_forward(c):
        wait_bytes(wout.at[:, pl.ds(0, 2 * cc)], gd_sem.at[c])
        for part, peer, origin in ((0, right, left), (1, left, right)):
            theirs = wout.at[pl.ds(part * thalf, thalf), cols(origin, c)]
            remote(theirs, theirs, gs_sem.at[c], gf_sem.at[c], samp=peer).start()

    def sweep_last(c, carry):
        @pl.when((c > 0) & (c <= GATHER_FIRST))
        def _():
            gather_direct(c - 1)

        sweep_chunk(c, resid_b)
        return carry

    lax.fori_loop(0, nch, sweep_last, 0)
    scatter_start(SWEEPS)

    def gather_more(c, carry):
        gather_direct(c)
        return carry

    lax.fori_loop(GATHER_FIRST, GATHER_AHEAD, gather_more, 0)
    rout_ref[...] = rs[s] - STEP_WEIGHT * sum_blocks(1, scatter_done(SWEEPS))

    def gather_step(c, carry):
        gather_forward(c)

        @pl.when(c + GATHER_AHEAD < nch)
        def _():
            gather_direct(c + GATHER_AHEAD)

        return carry

    lax.fori_loop(0, nch, gather_step, 0)

    def drain(c, carry):
        wait_bytes(xs.at[c, pl.ds(0, rows_all - rows)], xsend_sem.at[c])
        wait_bytes(wout.at[:, pl.ds(0, cc)], gf_sem.at[c])
        wait_bytes(wout.at[:, pl.ds(0, 3 * cc)], gs_sem.at[c])
        return carry

    lax.fori_loop(0, nch, drain, 0)
    for r in range(2):
        wait_bytes(p2.at[r, pl.ds(0, nf - 1)], p2s_sem.at[r])
    for r in range(SWEEPS - 1):
        wait_bytes(pm.at[r, pl.ds(0, ns * nf - 1)], pms_sem.at[r])
    for r in range(SWEEPS):
        wait_bytes(p1.at[r, pl.ds(0, ns - 1)], p1s_sem.at[r])


def solution(mesh):
    ns, nf = mesh.shape["samp"], mesh.shape["feat"]
    design_spec = P(("problem", "samp"), "feat")
    rows_spec = P(("problem", "samp"), None)
    coef_spec = P(("problem", "feat"), None)
    step_spec = P(("problem", "feat"))
    ridge_spec = P("problem")

    def local_sweeps(design, targets, coef_init, step_sizes, ridge_weights):
        rows, width = design.shape
        nt = targets.shape[1]
        quarter = width // ns
        nch = quarter // CHUNK
        dma = pltpu.SemaphoreType.DMA
        any_spec = pl.BlockSpec(memory_space=pl.ANY)
        vmem_spec = pl.BlockSpec(memory_space=pltpu.VMEM)
        coef_t, resid_t = pl.pallas_call(
            functools.partial(sweeps_kernel, ns, nf, rows * ns),
            out_shape=(pltpu.VMEM((nt, width), jnp.float32),
                       jax.ShapeDtypeStruct((nt, rows), jnp.float32)),
            in_specs=[any_spec, vmem_spec, any_spec, any_spec, vmem_spec],
            out_specs=(vmem_spec, vmem_spec),
            scratch_shapes=[
                pltpu.VMEM((nch, rows * ns, CHUNK), jnp.bfloat16),
                pltpu.VMEM((nch, nt, CHUNK), jnp.bfloat16),
                pltpu.VMEM((1, quarter), jnp.float32),
                pltpu.VMEM((nt, rows * ns), jnp.float32),
                pltpu.VMEM((STREAM_BUFS, rows, STREAM), jnp.bfloat16),
                pltpu.VMEM((STREAM_BUFS, nt, STREAM), jnp.float32),
                pltpu.VMEM((SWEEPS, ns, nt, rows), jnp.float32),
                pltpu.VMEM((SWEEPS, ns, nt, rows), jnp.float32),
                pltpu.VMEM((2, nf, nt, rows), jnp.bfloat16),
                pltpu.VMEM((SWEEPS - 1, ns * nf, nt, rows), jnp.bfloat16),
                pltpu.VMEM((ns, nt, rows), jnp.float32),
                dma((nch,)), dma((nch,)), dma((nch,)), dma, dma((STREAM_BUFS,)), dma((STREAM_BUFS,)),
                dma((SWEEPS,)), dma((SWEEPS,)), dma((2,)), dma((2,)), dma((SWEEPS - 1,)), dma((SWEEPS - 1,)), dma, dma,
                dma((nch,)), dma((nch,)), dma((nch,)),
            ],
            compiler_params=pltpu.CompilerParams(
                collective_id=0, has_side_effects=True, vmem_limit_bytes=47 * 1024 * 1024),
            name="sweeps",
        )(design, targets.T, coef_init.T, step_sizes[None, :], ridge_weights[None, :])
        return coef_t.T, resid_t.T

    return jax.shard_map(
        local_sweeps, mesh=mesh, in_specs=(design_spec, rows_spec, coef_spec, step_spec, ridge_spec),
        out_specs=(coef_spec, rows_spec), check_vma=False)
```

```python
import functools

import jax
import jax.numpy as jnp
from jax import lax
from jax.experimental import pallas as pl
from jax.experimental.pallas import tpu as pltpu
from jax.sharding import PartitionSpec as P

SWEEPS = 4
STEP_WEIGHT = 0.5
CHUNK = 2048
AHEAD = 4
STREAM = 4096
STREAM_BUFS = 3
GATHER_FIRST = 4
GATHER_AHEAD = 8
UNROLL = 8
MESH = pl.DeviceIdType.MESH


def sweeps_kernel(
    ns, nf, total_rows,
    x_hbm, y_ref, w0_hbm, eta_hbm, lam_ref,
    wout, rout_ref,
    xs, sb, eta, acc, sx, sw, p1s, p1, p2, pm, rs,
    x_sem, xsend_sem, w_sem, eta_sem, sx_sem, sw_sem,
    p1_sem, p1s_sem, p2_sem, p2s_sem, pm_sem, pms_sem, rs_sem, rss_sem,
    gd_sem, gf_sem, gs_sem,
):
    nch, rows_all, cc = xs.shape
    rows = rows_all // ns
    targets = y_ref.shape[0]
    thalf = targets // 2
    quarter = nch * cc
    nstream = x_hbm.shape[1] // STREAM
    s = lax.axis_index("samp")
    f = lax.axis_index("feat")
    right, left, opp = lax.rem(s + 1, ns), lax.rem(s + ns - 1, ns), lax.rem(s + 2, ns)
    samp_peers = [opp, right, left]
    feat_peers = [lax.rem(f + k, nf) for k in range(1, nf)]
    far_first = sorted(((i, j) for i in range(ns) for j in range(nf) if i or j),
                       key=lambda d: -min(d[0], ns - d[0]) - min(d[1], nf - d[1]) / 2)
    group = [{"samp": lax.rem(s + i, ns), "feat": lax.rem(f + j, nf)} for i, j in far_first]

    def remote(src, dst, send_sem, recv_sem, **where):
        return pltpu.make_async_remote_copy(
            src_ref=src, dst_ref=dst, send_sem=send_sem, recv_sem=recv_sem,
            device_id=where, device_id_type=MESH)

    def cols(owner, c):
        return pl.ds(pl.multiple_of(owner * quarter + c * cc, cc), cc)

    def wait_bytes(ref, sem):
        pltpu.make_async_copy(ref, ref, sem).wait()

    barrier = pltpu.get_barrier_semaphore()
    for peer in group:
        pl.semaphore_signal(barrier, inc=1, device_id=peer, device_id_type=MESH)
    pl.semaphore_wait(barrier, len(group))

    def issue(c):
        mine = pl.ds(pl.multiple_of(s * rows, rows), rows)
        for peer in (opp, right, left):
            remote(x_hbm.at[:, cols(peer, c)], xs.at[c, mine, :], xsend_sem.at[c], x_sem.at[c], samp=peer).start()
        pltpu.make_async_copy(x_hbm.at[:, cols(s, c)], xs.at[c, mine, :], x_sem.at[c]).start()
        pltpu.make_async_copy(w0_hbm.at[:, cols(s, c)], wout.at[:, cols(s, c)], w_sem.at[c]).start()

    def stream_copies(i):
        slot = lax.rem(i, STREAM_BUFS)
        span = pl.ds(pl.multiple_of(i * STREAM, STREAM), STREAM)
        return (pltpu.make_async_copy(x_hbm.at[:, span], sx.at[slot], sx_sem.at[slot]),
                pltpu.make_async_copy(w0_hbm.at[:, span], sw.at[slot], sw_sem.at[slot]))

    for i in range(STREAM_BUFS - 1):
        for copy in stream_copies(i):
            copy.start()

    def issue_step(c, carry):
        issue(c)
        return carry

    lax.fori_loop(0, AHEAD, issue_step, 0)
    eta_copy = pltpu.make_async_copy(
        eta_hbm.at[:, pl.ds(pl.multiple_of(s * quarter, quarter), quarter)], eta, eta_sem)
    eta_copy.start()

    contract_last = (((1,), (1,)), ((), ()))

    def first_product(i, total):
        @pl.when(i + STREAM_BUFS - 1 < nstream)
        def _():
            for copy in stream_copies(i + STREAM_BUFS - 1):
                copy.start()

        for copy in stream_copies(i):
            copy.wait()
        slot = lax.rem(i, STREAM_BUFS)
        return total + lax.dot_general(
            sw[slot].astype(jnp.bfloat16), sx[slot], contract_last, preferred_element_type=jnp.float32)

    block_rows = lax.fori_loop(0, nstream, first_product, jnp.zeros((targets, rows), jnp.float32))

    def sum_blocks(r, block_rows):
        p2[r, f] = block_rows.astype(jnp.bfloat16)
        copies = [remote(p2.at[r, f], p2.at[r, f], p2s_sem.at[r], p2_sem.at[r], feat=peer) for peer in feat_peers]
        for copy in copies:
            copy.start()
        wait_bytes(p2.at[r, pl.ds(0, nf - 1)], p2_sem.at[r])
        total = p2[r, 0].astype(jnp.float32)
        for j in range(1, nf):
            total = total + p2[r, j].astype(jnp.float32)
        return total

    def sum_blocks_all(r, block_rows):
        pm[r - 1, s * nf + f] = block_rows.astype(jnp.bfloat16)
        mine = pm.at[r - 1, s * nf + f]
        for peer in group:
            remote(mine, mine, pms_sem.at[r - 1], pm_sem.at[r - 1], **peer).start()
        wait_bytes(pm.at[r - 1, pl.ds(0, ns * nf - 1)], pm_sem.at[r - 1])
        for q in range(ns):
            total = pm[r - 1, q * nf].astype(jnp.float32)
            for j in range(1, nf):
                total = total + pm[r - 1, q * nf + j].astype(jnp.float32)
            rs[q] = rs[q] - STEP_WEIGHT * total

    def rounded_resid():
        return jnp.concatenate([rs[q].astype(jnp.bfloat16) for q in range(ns)], axis=1)

    def scatter_start(r):
        for q in range(ns):
            p1s[r - 1, q] = acc[:, q * rows:(q + 1) * rows]
        for peer in samp_peers:
            remote(p1s.at[r - 1, peer], p1.at[r - 1, s], p1s_sem.at[r - 1], p1_sem.at[r - 1], samp=peer).start()
        p1[r - 1, s] = p1s[r - 1, s]

    def scatter_done(r):
        wait_bytes(p1.at[r - 1, pl.ds(0, ns - 1)], p1_sem.at[r - 1])
        total = p1[r - 1, 0]
        for q in range(1, ns):
            total = total + p1[r - 1, q]
        return total

    rs[s] = y_ref[...] - sum_blocks(0, block_rows)
    for peer in samp_peers:
        remote(rs.at[s], rs.at[s], rss_sem, rs_sem, samp=peer).start()
    wait_bytes(rs.at[pl.ds(0, ns - 1)], rs_sem)
    wait_bytes(rs.at[pl.ds(0, ns - 1)], rss_sem)
    resid_b = rounded_resid()

    diag = lax.broadcasted_iota(jnp.int32, (targets, targets), 0) == lax.broadcasted_iota(
        jnp.int32, (targets, targets), 1)
    ridge = jnp.sum(jnp.where(diag, jnp.broadcast_to(lam_ref[...], (targets, targets)), 0.0), axis=1, keepdims=True)
    eta_copy.wait()

    def sweep_chunk(c, resid_b):
        xc = xs[c]
        grad = jnp.dot(resid_b, xc, preferred_element_type=jnp.float32) / total_rows
        w = wout[:, cols(s, c)]
        step = eta[:, pl.ds(pl.multiple_of(c * cc, cc), cc)] * (grad - ridge * w)
        wout[:, cols(s, c)] = w + STEP_WEIGHT * step
        acc[...] += lax.dot_general(step.astype(jnp.bfloat16), xc, contract_last, preferred_element_type=jnp.float32)

    acc[...] = jnp.zeros_like(acc)

    def sweep_first(c, carry):
        @pl.when(c + AHEAD < nch)
        def _():
            issue(c + AHEAD)

        wait_bytes(xs.at[c], x_sem.at[c])
        wait_bytes(wout.at[:, pl.ds(0, cc)], w_sem.at[c])
        sweep_chunk(c, resid_b)
        return carry

    lax.fori_loop(0, nch, sweep_first, 0)

    def later_sweep(r, resid_b):
        def step_chunk(c, carry):
            if r == SWEEPS:
                @pl.when((c > 0) & (c <= GATHER_FIRST))
                def _():
                    gather_direct(c - 1)

            grad = jnp.dot(resid_b, xs[c], preferred_element_type=jnp.float32) / total_rows
            w = wout[:, cols(s, c)]
            step = eta[:, pl.ds(pl.multiple_of(c * cc, cc), cc)] * (grad - ridge * w)
            wout[:, cols(s, c)] = w + STEP_WEIGHT * step
            sb[c] = step.astype(jnp.bfloat16)
            return carry

        lax.fori_loop(0, nch, step_chunk, 0, unroll=UNROLL)

        def block_product(q):
            block = pl.ds(pl.multiple_of(q * rows, rows), rows)
            total = jnp.zeros((rows, targets), jnp.float32)
            for c in range(nch):
                total = total + lax.dot_general(xs[c, block, :], sb[c], contract_last, preferred_element_type=jnp.float32)
            return total.T

        def peer_block(p, carry):
            q = lax.rem(s + 1 + p, ns)
            p1s[r - 1, q] = block_product(q)
            remote(p1s.at[r - 1, q], p1.at[r - 1, s], p1s_sem.at[r - 1], p1_sem.at[r - 1], samp=q).start()
            return carry

        lax.fori_loop(0, ns - 1, peer_block, 0)
        p1[r - 1, s] = block_product(s)

    scatter_start(1)
    sum_blocks_all(1, scatter_done(1))
    for r in range(2, SWEEPS):
        later_sweep(r, rounded_resid())
        sum_blocks_all(r, scatter_done(r))

    def gather_direct(c):
        mine = wout.at[:, cols(s, c)]
        for peer in (right, left):
            remote(mine, mine, gs_sem.at[c], gd_sem.at[c], samp=peer).start()

    def gather_forward(c):
        wait_bytes(wout.at[:, pl.ds(0, 2 * cc)], gd_sem.at[c])
        for part, peer, origin in ((0, right, left), (1, left, right)):
            theirs = wout.at[pl.ds(part * thalf, thalf), cols(origin, c)]
            remote(theirs, theirs, gs_sem.at[c], gf_sem.at[c], samp=peer).start()

    later_sweep(SWEEPS, rounded_resid())

    def gather_more(c, carry):
        gather_direct(c)
        return carry

    lax.fori_loop(GATHER_FIRST, GATHER_AHEAD, gather_more, 0)
    rout_ref[...] = rs[s] - STEP_WEIGHT * sum_blocks(1, scatter_done(SWEEPS))

    def gather_step(c, carry):
        gather_forward(c)

        @pl.when(c + GATHER_AHEAD < nch)
        def _():
            gather_direct(c + GATHER_AHEAD)

        return carry

    lax.fori_loop(0, nch, gather_step, 0)

    def drain(c, carry):
        wait_bytes(xs.at[c, pl.ds(0, rows_all - rows)], xsend_sem.at[c])
        wait_bytes(wout.at[:, pl.ds(0, cc)], gf_sem.at[c])
        wait_bytes(wout.at[:, pl.ds(0, 3 * cc)], gs_sem.at[c])
        return carry

    lax.fori_loop(0, nch, drain, 0)
    for r in range(2):
        wait_bytes(p2.at[r, pl.ds(0, nf - 1)], p2s_sem.at[r])
    for r in range(SWEEPS - 1):
        wait_bytes(pm.at[r, pl.ds(0, ns * nf - 1)], pms_sem.at[r])
    for r in range(SWEEPS):
        wait_bytes(p1.at[r, pl.ds(0, ns - 1)], p1s_sem.at[r])


def solution(mesh):
    ns, nf = mesh.shape["samp"], mesh.shape["feat"]
    design_spec = P(("problem", "samp"), "feat")
    rows_spec = P(("problem", "samp"), None)
    coef_spec = P(("problem", "feat"), None)
    step_spec = P(("problem", "feat"))
    ridge_spec = P("problem")

    def local_sweeps(design, targets, coef_init, step_sizes, ridge_weights):
        rows, width = design.shape
        nt = targets.shape[1]
        quarter = width // ns
        nch = quarter // CHUNK
        dma = pltpu.SemaphoreType.DMA
        any_spec = pl.BlockSpec(memory_space=pl.ANY)
        vmem_spec = pl.BlockSpec(memory_space=pltpu.VMEM)
        coef_t, resid_t = pl.pallas_call(
            functools.partial(sweeps_kernel, ns, nf, rows * ns),
            out_shape=(pltpu.VMEM((nt, width), jnp.float32),
                       jax.ShapeDtypeStruct((nt, rows), jnp.float32)),
            in_specs=[any_spec, vmem_spec, any_spec, any_spec, vmem_spec],
            out_specs=(vmem_spec, vmem_spec),
            scratch_shapes=[
                pltpu.VMEM((nch, rows * ns, CHUNK), jnp.bfloat16),
                pltpu.VMEM((nch, nt, CHUNK), jnp.bfloat16),
                pltpu.VMEM((1, quarter), jnp.float32),
                pltpu.VMEM((nt, rows * ns), jnp.float32),
                pltpu.VMEM((STREAM_BUFS, rows, STREAM), jnp.bfloat16),
                pltpu.VMEM((STREAM_BUFS, nt, STREAM), jnp.float32),
                pltpu.VMEM((SWEEPS, ns, nt, rows), jnp.float32),
                pltpu.VMEM((SWEEPS, ns, nt, rows), jnp.float32),
                pltpu.VMEM((2, nf, nt, rows), jnp.bfloat16),
                pltpu.VMEM((SWEEPS - 1, ns * nf, nt, rows), jnp.bfloat16),
                pltpu.VMEM((ns, nt, rows), jnp.float32),
                dma((nch,)), dma((nch,)), dma((nch,)), dma, dma((STREAM_BUFS,)), dma((STREAM_BUFS,)),
                dma((SWEEPS,)), dma((SWEEPS,)), dma((2,)), dma((2,)), dma((SWEEPS - 1,)), dma((SWEEPS - 1,)), dma, dma,
                dma((nch,)), dma((nch,)), dma((nch,)),
            ],
            compiler_params=pltpu.CompilerParams(
                collective_id=0, has_side_effects=True, vmem_limit_bytes=47 * 1024 * 1024),
            name="sweeps",
        )(design, targets.T, coef_init.T, step_sizes[None, :], ridge_weights[None, :])
        return coef_t.T, resid_t.T

    return jax.shard_map(
        local_sweeps, mesh=mesh, in_specs=(design_spec, rows_spec, coef_spec, step_spec, ridge_spec),
        out_specs=(coef_spec, rows_spec), check_vma=False)
```
